512 devices in a mesh: groups: 2 (over y), seq: 32 (over z), head: 8 (over x, core).
Axes of the slice: x: 4, y: 2, z: 32, core: 2. Of those that a mesh axis runs over, the one named last changes fastest.
The devices are a block of a 4x8x32 slice.
Arguments:
- queries: bfloat16 [16384, 8192], P(('groups', 'seq'), 'head'), parts along dimension 0, may hold values from -16 to 16
- keys: bfloat16 [16384, 1024], P(('groups', 'seq'), 'head'), parts along dimension 0, may hold values from -16 to 16
- values: bfloat16 [16384, 1024], P(('groups', 'seq'), 'head'), parts along dimension 0, may hold values from -6 to 6
- prompt_len: int32 [2], P('groups'), parts along dimension 0, may hold values from 2048 to 8192
- page_dest: int32 [64, 2], P('groups'), parts along dimension 0, may hold values from 0 to 31, all different within a row; in each aligned block of 32 rows (0 to 31, 32 to 63, ...) at most 4 rows name the same one
Outputs:
- attended: bfloat16 [16384, 8192], P(('groups', 'seq'), 'head'), parts along dimension 0
- decode_page_cache: bfloat16 [256, 128, 2048], P(('groups', 'seq'), None, 'head'), parts along dimension 0
The draws below stay inside these ranges and needn't reach their ends.
There are 2 independent parts, one for each index of `groups`. The reference program is written for one: setup_inputs(seed, part) draws one part's arguments, and reference() takes and returns one part's arrays. A program takes and returns all parts, laid end to end along the dimension named above; each array names one. Nothing has to cross between parts.
Inputs may be any that keep to these rules, and one draw needn't show every extreme that they name: `page_dest`: row s names the decode devices of the 2 pages of tokens s * 256 to (s + 1) * 256 - 1, all different within a row; no device is named more than 4 times in all, and some device exactly 4 times.
All inputs are finite; a program needn't handle non-finite values.
Results may differ from the reference program's by a relative error of at most 0.005.
Values may be sent and summed in bfloat16 or wider, within the bound.
No kernel may reach another device: no remote copies, remote signals or barrier semaphores. Data moves between devices by JAX's collectives and lax.ppermute only.
A program may use at most 64 MiB of HBM per device.

```python
import math
import jax
import jax.numpy as jnp
import numpy as np
from jax import lax

QUERY_HEADS = 64
KEY_VALUE_HEADS = 8
HEAD_SIZE = 128
PAGE_TOKENS = 128
QUERY_PER_KV = 8
PROMPT_TOKENS = 8192
PPD = 2
DEVICE_SLOTS = 4
PROMPT_PAGES = 64
N_SEQ = 32


def starting_rows(key, columns):
    return jnp.clip(jax.random.normal(jax.random.fold_in(key, 13), (PROMPT_TOKENS, columns), jnp.float32), -4.0, 4.0)


def draw_queries(key, part):
    sampled_inputs = starting_rows(jax.random.fold_in(key, 21), QUERY_HEADS * HEAD_SIZE)
    return sampled_inputs.astype(jnp.bfloat16)


def draw_keys(key, part):
    sampled_inputs = starting_rows(jax.random.fold_in(key, 22), KEY_VALUE_HEADS * HEAD_SIZE)
    return sampled_inputs.astype(jnp.bfloat16)


def steps_of(stream_key, shape, split, smallest, high):
    def one(position, parts):
        heights = jax.random.uniform(jax.random.fold_in(jax.random.fold_in(stream_key, 6), position), (parts,), jnp.float32, smallest / len(split), high / len(split))
        return jnp.repeat(jnp.exp(heights), shape[position] // parts).reshape((-1,) + (1,) * (len(shape) - position - 1))

    loudness = one(*split[0])
    for cut in split[1:]:
        loudness = loudness * one(*cut)
    return loudness


def deal_out(stream_key, own, number, rows, amount, top, most, slope):
    order = jax.random.permutation(stream_key, amount)
    packed, ordinary = portions_of(amount, rows * top, most, slope, True), portions_of(amount, rows * top, most, slope, False)
    places = jnp.arange(amount)

    def named(tallies, rotation):
        used = int((tallies > 0).sum())
        fixed = max(1, used // 4)
        passed = fixed + (places - fixed + rotation * (used - fixed)) % max(1, amount - fixed)
        return jnp.zeros((amount,), jnp.int32).at[order[jnp.where(places < fixed, places, passed)]].set(jnp.asarray(tallies, jnp.int32))

    tallies = jnp.where(number % 4 == 0, named(packed, number // 4), named(ordinary, number - number // 4 - 1))
    mixed = jax.random.permutation(jax.random.fold_in(own, 3), amount)
    source_of, receiver = mixed[0:amount // 2 * 2:2], mixed[1:amount // 2 * 2:2]
    room = jnp.minimum(tallies[source_of] - 1, most - tallies[receiver]) // 2
    room = jnp.where((source_of == order[0]) | (receiver == order[0]) | (tallies[receiver] == 0), 0, jnp.maximum(room, 0))
    passed = jax.random.randint(jax.random.fold_in(own, 4), (amount // 2,), 0, 1 << 20) % (room + 1)
    tallies = tallies.at[source_of].add(-passed).at[receiver].add(passed)
    members = jnp.searchsorted(jnp.cumsum(tallies), jnp.arange(rows * top), side="right").astype(jnp.int32)
    listing = members.reshape(top, rows).T
    listing = listing[jax.random.permutation(jax.random.fold_in(own, 1), rows)]
    rotation = jax.random.randint(jax.random.fold_in(own, 2), (rows, 1), 0, top)
    return jnp.take_along_axis(listing, (jnp.arange(top)[None, :] + rotation) % top, axis=1)


def portions_of(amount, total, limit, slope, full):
    portions = [(1 << 20) // math.isqrt(grade ** slope) + 1 for grade in range(1, amount + 1)]
    largest = limit if full else min(limit, max(-(-total // amount), total * portions[0] // sum(portions)))
    least = 1 if total - largest >= amount - 1 else 0
    counts, spare = [largest] + [least] * (amount - 1), total - largest - least * (amount - 1)
    while spare > 0:
        candidates = [i for i in range(1, amount) if counts[i] < largest] or [i for i in range(1, amount) if counts[i] < limit]
        pool, remaining = sum([portions[i] for i in candidates]), spare
        for i in candidates:
            addition = min(limit - counts[i], max(1, remaining * portions[i] // pool), spare)
            counts[i] = counts[i] + addition
            spare = spare - addition
    return np.array(counts)


def gaussian(stream_key, dims, width, reach, pieces=(), kind=jnp.bfloat16):
    drawn = jax.random.normal(stream_key, dims, jnp.float32) * width
    if len(pieces) > 0:
        drawn = steps_of(stream_key, dims, pieces, -0.22, 0.18) * drawn
    return jnp.clip(drawn, min=-reach, max=reach).astype(kind)


def setup_inputs(seed: int = 0, part: int = 0) -> dict:
    splits = jax.random.split(jax.random.key(seed), 6)
    part_splits = jax.random.split(jax.random.fold_in(splits[5], part), 6)
    queries = draw_queries(jax.random.fold_in(jax.random.fold_in(splits[5], part), 71), part)
    keys = draw_keys(jax.random.fold_in(jax.random.fold_in(splits[5], part), 71), part)
    values = gaussian(part_splits[2], (PROMPT_TOKENS, KEY_VALUE_HEADS * HEAD_SIZE), 1.0, 6.0, ((0, 32), (1, 8)))
    prompt_len = jax.random.randint(part_splits[3], (1,), PROMPT_TOKENS // 4, PROMPT_TOKENS + 1).astype(jnp.int32)
    page_dest_keys = jax.random.split(jax.random.fold_in(part_splits[4], 1), N_SEQ // N_SEQ)
    page_dest_turns = jax.random.permutation(jax.random.fold_in(part_splits[4], 3), N_SEQ // N_SEQ)
    page_dest = jax.vmap(lambda own, number: deal_out(jax.random.fold_in(part_splits[4], 2), own, number, N_SEQ, N_SEQ, PPD, DEVICE_SLOTS, 2))(page_dest_keys, page_dest_turns).reshape((N_SEQ, PPD))
    return {"queries": queries, "keys": keys, "values": values, "prompt_len": prompt_len, "page_dest": page_dest}


NEG_FILL = -1e+30

def reference(queries, keys, values, prompt_len, page_dest):
    prompt_end = prompt_len[0]
    score_scale = 1.0 / math.sqrt(HEAD_SIZE)
    rows_in_block = math.gcd(PROMPT_TOKENS, 256)
    blocks = PROMPT_TOKENS // rows_in_block
    positions = jnp.arange(PROMPT_TOKENS, dtype=jnp.int32)
    key_live = positions < prompt_end
    key_head_rows = keys.reshape(PROMPT_TOKENS, KEY_VALUE_HEADS, HEAD_SIZE).transpose(1, 0, 2).astype(jnp.float32)
    value_head_rows = values.reshape(PROMPT_TOKENS, KEY_VALUE_HEADS, HEAD_SIZE).transpose(1, 0, 2).astype(jnp.float32)

    def query_block(number):
        first_row = (number * rows_in_block).astype(jnp.int32)
        query_block_rows = lax.dynamic_slice_in_dim(queries, first_row, rows_in_block, 0)
        query_block_rows = query_block_rows.reshape(rows_in_block, KEY_VALUE_HEADS, QUERY_PER_KV, HEAD_SIZE).transpose(1, 2, 0, 3).astype(jnp.float32)
        query_pos = first_row + jnp.arange(rows_in_block, dtype=jnp.int32)
        allowed = (positions[None, :] <= query_pos[:, None]) & key_live[None, :]
        query_live = query_pos < prompt_end

        def one_head(head_items):
            head_rows, head_keys, head_values = head_items
            scores = jnp.einsum('grd,pd->grp', head_rows, head_keys) * score_scale
            scores = jnp.where(allowed[None], scores, NEG_FILL)
            row_max = lax.optimization_barrier(jnp.max(scores, axis=-1, keepdims=True))
            weights = jnp.where(allowed[None], jnp.exp(scores - row_max), 0.0)
            denominator = lax.optimization_barrier(jnp.sum(weights, axis=-1))
            rounded = lax.optimization_barrier(weights.astype(jnp.bfloat16)).astype(jnp.float32)
            weighted = jnp.einsum('grp,pd->grd', rounded, head_values)
            safe_total = jnp.where(query_live[None, :], denominator, 1.0)
            return jnp.where(query_live[None, :, None], weighted / safe_total[..., None], 0.0)
        result = lax.map(one_head, (query_block_rows, key_head_rows, value_head_rows))
        return result.transpose(2, 0, 1, 3).reshape(rows_in_block, QUERY_HEADS * HEAD_SIZE).astype(jnp.bfloat16)
    attended = lax.map(query_block, jnp.arange(blocks, dtype=jnp.int32)).reshape(PROMPT_TOKENS, QUERY_HEADS * HEAD_SIZE)
    flat_dest = page_dest.reshape(-1).astype(jnp.int32)
    page_order = jnp.arange(PROMPT_PAGES, dtype=jnp.int32)
    same_dest = flat_dest[:, None] == flat_dest[None, :]
    dest_rank = lax.optimization_barrier(jnp.sum(same_dest & (page_order[None, :] < page_order[:, None]), axis=1)).astype(jnp.int32)
    target_slot_index = (flat_dest * DEVICE_SLOTS + dest_rank).astype(jnp.int32)
    token_present = key_live[:, None]
    retained_keys = jnp.where(token_present, keys, jnp.zeros((), jnp.bfloat16)).reshape(PROMPT_PAGES, PAGE_TOKENS, KEY_VALUE_HEADS, HEAD_SIZE)
    retained_values = jnp.where(token_present, values, jnp.zeros((), jnp.bfloat16)).reshape(PROMPT_PAGES, PAGE_TOKENS, KEY_VALUE_HEADS, HEAD_SIZE)
    page_content = jnp.stack((retained_keys, retained_values), axis=3).reshape(PROMPT_PAGES, PAGE_TOKENS, 2 * KEY_VALUE_HEADS * HEAD_SIZE)
    decode_page_cache = jnp.zeros((N_SEQ * DEVICE_SLOTS, PAGE_TOKENS, 2 * KEY_VALUE_HEADS * HEAD_SIZE), jnp.bfloat16).at[target_slot_index].set(page_content)
    return (attended, decode_page_cache)
```

```python
import math

import jax
import jax.numpy as jnp
from jax import lax
from jax.experimental import pallas as pl
from jax.experimental.pallas import tpu as pltpu
from jax.sharding import PartitionSpec as P

HEAD_SIZE = 128
PAGE_TOKENS = 128
ONES_ROWS = 16
NEG_FILL = -1e30
SHIFT_LIMIT = 64.0
AHEAD = 3
LAG = 1
EXP2_SCALE = math.log2(math.e) / math.sqrt(HEAD_SIZE)


def values_across(v):
    turned = v.astype(jnp.float32).T.astype(jnp.bfloat16)
    return jnp.concatenate([turned, jnp.ones((ONES_ROWS, v.shape[0]), jnp.bfloat16)], axis=0)


def store_pages(meta, pages, piece, row0, number, rows):
    for k in range(rows // PAGE_TOKENS):
        slot = meta[2 + number * (rows // PAGE_TOKENS) + k]

        @pl.when(slot >= 0)
        def _():
            first = number * rows + k * PAGE_TOKENS
            token = first + lax.broadcasted_iota(jnp.int32, (PAGE_TOKENS, 2 * HEAD_SIZE), 0)
            block = piece[pl.ds(row0 + k * PAGE_TOKENS, PAGE_TOKENS), :]
            kept = jnp.where(token < meta[1], block.astype(jnp.float32), 0.0)
            pages[pl.ds(slot, 1)] = kept.astype(jnp.bfloat16)[None]


def attend(q_ref, m_ref, acc_ref, k_ref, v_ref, which, heads):
    for h in range(heads):
        q = q_ref[h]
        scores = [jnp.dot(k_ref[i], q, preferred_element_type=jnp.float32) for i in which]
        old = m_ref[h : h + 1, :]
        new = old
        for s in scores:
            new = jnp.maximum(new, jnp.max(s, axis=0, keepdims=True))
        shift = new * EXP2_SCALE
        total = acc_ref[h] * jnp.exp2(old * EXP2_SCALE - shift)
        for s, i in zip(scores, which):
            w = jnp.exp2(s * EXP2_SCALE - shift).astype(jnp.bfloat16)
            total = total + jnp.dot(v_ref[i], w, preferred_element_type=jnp.float32)
        m_ref[h : h + 1, :] = new
        acc_ref[h] = total


def first_kernel(meta, queries, piece, q_ref, m_ref, acc_ref, pages, *, heads, rows):
    pages[...] = jnp.zeros_like(pages)
    store_pages(meta, pages, piece, 0, meta[0], rows)

    @pl.when(meta[0] * rows < meta[1])
    def _():
        k = piece[:, :HEAD_SIZE]
        v = values_across(piece[:, HEAD_SIZE:])
        key = lax.broadcasted_iota(jnp.int32, (rows, rows), 0)
        query = lax.broadcasted_iota(jnp.int32, (rows, rows), 1)
        allowed = key <= query
        for h in range(heads):
            q = queries[:, h * HEAD_SIZE : (h + 1) * HEAD_SIZE]
            q = q.astype(jnp.float32).T.astype(jnp.bfloat16)
            q_ref[h] = q
            s = jnp.dot(k, q, preferred_element_type=jnp.float32)
            s = jnp.where(allowed, s, NEG_FILL)
            new = jnp.max(s, axis=0, keepdims=True)
            w = jnp.exp2((s - new) * EXP2_SCALE).astype(jnp.bfloat16)
            m_ref[h : h + 1, :] = new
            acc_ref[h] = jnp.dot(v, w, preferred_element_type=jnp.float32)


def run_batches(
    meta, q_ref, m_in, acc_in, m_ref, acc_ref, pages, pieces, offsets, k_ref, v_ref, want,
    heads, rows, shards,
):
    live = meta[0] * rows < meta[1]
    parts, needed = [], []
    for ref, offs in zip(pieces, offsets):
        for i, off in enumerate(offs):
            if off is not None:
                number = lax.rem(meta[0] + (off % shards), shards)
                store_pages(meta, pages, ref, i * rows, number, rows)
                parts.append((ref, i * rows))
                needed.append(jnp.logical_and(number < meta[0], live))
    total = len(parts)
    some = needed[0]
    for n in needed[1:]:
        some = jnp.logical_or(some, n)
    m_ref[...] = m_in[...]

    @pl.when(jnp.logical_not(some))
    def _():
        acc_ref[...] = acc_in[...]

    @pl.when(some)
    def _():
        skip = []
        for i, (ref, row0) in enumerate(parts):
            v_ref[i] = values_across(ref[row0 : row0 + rows, HEAD_SIZE:])
            skip.append(jnp.where(needed[i], 0.0, -NEG_FILL))
        units = [(i, h) for i in range(total) for h in range(heads)]
        worst = jnp.zeros((1, rows), jnp.float32)

        def scored(unit):
            (ref, row0), h = parts[unit[0]], unit[1]
            k = ref[row0 : row0 + rows, :HEAD_SIZE]
            return jnp.dot(k, q_ref[h], preferred_element_type=jnp.float32)

        ahead = [scored(u) for u in units[:AHEAD]]
        weights = []
        for n in range(len(units) + LAG):
            if n + AHEAD < len(units):
                ahead.append(scored(units[n + AHEAD]))
            if n < len(units):
                i, h = units[n]
                t = ahead[n] * EXP2_SCALE - (m_in[h : h + 1, :] * EXP2_SCALE + skip[i])
                ahead[n] = None
                worst = jnp.maximum(worst, jnp.max(t, axis=0, keepdims=True))
                weights.append(jnp.exp2(t).astype(jnp.bfloat16))
            if n >= LAG:
                i, h = units[n - LAG]
                base = acc_in[h] if i == 0 else acc_ref[h]
                got = jnp.dot(v_ref[i], weights[n - LAG], preferred_element_type=jnp.float32)
                weights[n - LAG] = None
                acc_ref[h] = base + got

        @pl.when(jnp.max(worst) > SHIFT_LIMIT)
        def _():
            acc_ref[...] = acc_in[...]
            for i, (ref, row0) in enumerate(parts):
                k_ref[i] = ref[row0 : row0 + rows, :HEAD_SIZE]
                want[i] = needed[i].astype(jnp.int32)

            def one(i, carry):
                @pl.when(want[i] == 1)
                def _():
                    attend(q_ref, m_ref, acc_ref, k_ref, v_ref, [i], heads)

                return carry

            lax.fori_loop(0, total, one, 0)


def step_kernel(*refs, offsets, heads, rows, shards, last):
    count = len(offsets)
    meta, q_ref, m_in, acc_in, pages_in = refs[:5]
    pieces = refs[5 : 5 + count]
    if last:
        out, pages, m_ref, acc_ref, k_ref, v_ref, want = refs[5 + count :]
    else:
        m_ref, acc_ref, pages, k_ref, v_ref, want = refs[5 + count :]
    pages[...] = pages_in[...]
    run_batches(
        meta, q_ref, m_in, acc_in, m_ref, acc_ref, pages, pieces, offsets, k_ref, v_ref, want,
        heads, rows, shards,
    )
    if last:
        row = meta[0] * rows + lax.broadcasted_iota(jnp.int32, (rows, HEAD_SIZE), 0)
        for h in range(heads):
            got = acc_ref[h, :HEAD_SIZE, :] / acc_ref[h, HEAD_SIZE : HEAD_SIZE + 1, :]
            got = jnp.where(row < meta[1], got.T, 0.0)
            out[:, h * HEAD_SIZE : (h + 1) * HEAD_SIZE] = got.astype(jnp.bfloat16)


SMEM = pl.BlockSpec(memory_space=pltpu.SMEM)
VMEM = pl.BlockSpec(memory_space=pltpu.VMEM)


def state_shapes(heads, rows, slots):
    return (
        pltpu.VMEM((heads, rows), jnp.float32),
        pltpu.VMEM((heads, HEAD_SIZE + ONES_ROWS, rows), jnp.float32),
        pltpu.VMEM((slots, PAGE_TOKENS, 2 * HEAD_SIZE), jnp.bfloat16),
    )


def near(x):
    return pltpu.with_memory_space_constraint(x, pltpu.VMEM)


def cost(heads, rows, pieces):
    return pl.CostEstimate(
        flops=4 * heads * rows * rows * pieces * HEAD_SIZE * 4,
        bytes_accessed=4 * 2**20,
        transcendentals=heads * rows * rows * pieces,
    )


def call_first(meta, queries, piece, heads, rows, slots):
    return pl.pallas_call(
        lambda *r: first_kernel(*r, heads=heads, rows=rows),
        in_specs=[SMEM, VMEM, VMEM],
        out_specs=[VMEM] * 4,
        out_shape=(pltpu.VMEM((heads, HEAD_SIZE, rows), jnp.bfloat16),)
        + state_shapes(heads, rows, slots),
        cost_estimate=cost(heads, rows, 1),
        compiler_params=pltpu.CompilerParams(vmem_limit_bytes=16 * 2**20),
        name="first",
    )(meta, queries, piece)


def call_step(meta, q, state, batches, heads, rows, slots, shards, last=False):
    pieces = [b for b, unused in batches]
    offsets = [o for unused, o in batches]
    shapes = state_shapes(heads, rows, slots)
    count = sum(o is not None for offs in offsets for o in offs)
    scratch = [
        pltpu.VMEM((count, rows, HEAD_SIZE), jnp.bfloat16),
        pltpu.VMEM((count, HEAD_SIZE + ONES_ROWS, rows), jnp.bfloat16),
        pltpu.SMEM((count,), jnp.int32),
    ]
    extra = {}
    if last:
        out_shape = (
            jax.ShapeDtypeStruct((rows, heads * HEAD_SIZE), jnp.bfloat16),
            jax.ShapeDtypeStruct((slots, PAGE_TOKENS, 2 * HEAD_SIZE), jnp.bfloat16),
        )
        scratch = [
            shapes[0],
            shapes[1],
        ] + scratch
    else:
        out_shape = shapes
    return pl.pallas_call(
        lambda *r: step_kernel(
            *r, offsets=offsets, heads=heads, rows=rows, shards=shards, last=last
        ),
        in_specs=[SMEM] + [VMEM] * (4 + len(pieces)),
        out_specs=[VMEM] * len(out_shape),
        out_shape=out_shape,
        cost_estimate=cost(heads, rows, count),
        scratch_shapes=scratch,
        compiler_params=pltpu.CompilerParams(vmem_limit_bytes=16 * 2**20),
        name="step",
        **extra,
    )(meta, near(q), *map(near, state), *map(near, pieces))


def slot_of_pages(page_dest, owner, prompt_len):
    flat = page_dest.reshape(-1)
    order = jnp.arange(flat.shape[0], dtype=jnp.int32)
    before = (flat[:, None] == flat[None, :]) & (order[None, :] < order[:, None])
    rank = jnp.sum(before.astype(jnp.int32), axis=1)
    slot = jnp.where(flat == owner, rank, -1)
    return jnp.concatenate([jnp.stack([owner, prompt_len[0]]), slot]).astype(jnp.int32)


def local(queries, keys, values, prompt_len, page_dest):
    rows = queries.shape[0]
    heads = queries.shape[1] // keys.shape[1]
    shards = page_dest.shape[0]
    slots = 2 * page_dest.shape[1]
    meta = slot_of_pages(page_dest, lax.axis_index("seq"), prompt_len)

    def moved(x, by):
        pairs = [(i, (i + by) % shards) for i in range(shards)]
        return lax.ppermute(x, "seq", pairs)

    own = jnp.concatenate([keys, values], axis=1)
    q, *state = call_first(meta, queries, own, heads, rows, slots)
    stride, steps = 3, shards // 6
    up = down = own
    pending = []
    seen = {0}

    def fresh(offs):
        kept = [None if o % shards in seen else o for o in offs]
        seen.update(o % shards for o in offs)
        return kept

    for t in range(1, steps + 1):
        up, down = moved(up, stride), moved(down, -stride)
        here = [-stride * t, stride * t]
        batch = [up, down]
        offs = list(here)
        if t == 1:
            batch, offs = [own] + batch, [0] + offs
        block = jnp.concatenate(batch, axis=0)
        from_below, from_above = moved(block, 1), moved(block, -1)
        todo = pending + [(up, fresh(here[:1])), (down, fresh(here[1:]))]
        state = call_step(meta, q, state, todo, heads, rows, slots, shards)
        below = fresh([o - 1 for o in offs])
        above = fresh([o + 1 for o in offs])
        pending = [(from_below, below), (from_above, above)]
    attended, pages = call_step(meta, q, state, pending, heads, rows, slots, shards, last=True)
    return attended, pages


def solution(mesh):
    return jax.shard_map(
        local,
        mesh=mesh,
        in_specs=(
            P(("groups", "seq"), "head"),
            P(("groups", "seq"), "head"),
            P(("groups", "seq"), "head"),
            P("groups"),
            P("groups", None),
        ),
        out_specs=(P(("groups", "seq"), "head"), P(("groups", "seq"), None, "head")),
        check_vma=False,
    )
```

```python
import math

import jax
import jax.numpy as jnp
from jax import lax
from jax.experimental import pallas as pl
from jax.experimental.pallas import tpu as pltpu
from jax.sharding import PartitionSpec as P

HEAD_SIZE = 128
PAGE_TOKENS = 128
ONES_ROWS = 16
NEG_FILL = -1e30
SHIFT_LIMIT = 64.0
AHEAD = 3
LAG = 1
PART = 4
EXP2_SCALE = math.log2(math.e) / math.sqrt(HEAD_SIZE)


def values_across(v):
    turned = v.astype(jnp.float32).T.astype(jnp.bfloat16)
    return jnp.concatenate([turned, jnp.ones((ONES_ROWS, v.shape[0]), jnp.bfloat16)], axis=0)


def attend(q_ref, m_ref, acc_ref, k_ref, v_ref, heads):
    for h in range(heads):
        s = jnp.dot(k_ref[...], q_ref[h], preferred_element_type=jnp.float32)
        old = m_ref[h : h + 1, :]
        new = jnp.maximum(old, jnp.max(s, axis=0, keepdims=True))
        shift = new * EXP2_SCALE
        w = jnp.exp2(s * EXP2_SCALE - shift).astype(jnp.bfloat16)
        got = jnp.dot(v_ref[...], w, preferred_element_type=jnp.float32)
        acc_ref[h] = acc_ref[h] * jnp.exp2(old * EXP2_SCALE - shift) + got
        m_ref[h : h + 1, :] = new


def own_tokens(queries, piece, q_ref, m_ref, acc_ref, heads, rows):
    k = piece[:, :HEAD_SIZE]
    v = values_across(piece[:, HEAD_SIZE:])
    key = lax.broadcasted_iota(jnp.int32, (rows, rows), 0)
    query = lax.broadcasted_iota(jnp.int32, (rows, rows), 1)
    allowed = key <= query
    for h in range(heads):
        q = queries[:, h * HEAD_SIZE : (h + 1) * HEAD_SIZE]
        q = q.astype(jnp.float32).T.astype(jnp.bfloat16)
        q_ref[h] = q
        s = jnp.dot(k, q, preferred_element_type=jnp.float32)
        s = jnp.where(allowed, s, NEG_FILL)
        new = jnp.max(s, axis=0, keepdims=True)
        w = jnp.exp2((s - new) * EXP2_SCALE).astype(jnp.bfloat16)
        m_ref[h : h + 1, :] = new
        acc_ref[h] = jnp.dot(v, w, preferred_element_type=jnp.float32)


def first_kernel(
    place, queries_hbm, keys, values, piece, q_ref, m_ref, acc_ref, queries, sems,
    *, heads, rows, shards,
):
    key_copy = pltpu.make_async_copy(keys, piece.at[:, pl.ds(0, HEAD_SIZE)], sems.at[0])
    value_copy = pltpu.make_async_copy(values, piece.at[:, pl.ds(HEAD_SIZE, HEAD_SIZE)], sems.at[1])
    key_copy.start()
    value_copy.start()
    key_copy.wait()
    value_copy.wait()

    @pl.when(place[0] < shards // 2)
    def _():
        pltpu.sync_copy(queries_hbm, queries)
        own_tokens(queries, piece, q_ref, m_ref, acc_ref, heads, rows)


def rest_kernel(*refs, offsets, heads, rows, shards, slots):
    count = len(offsets)
    meta, queries_hbm, q_first, m_first, acc_first = refs[:5]
    buffers = refs[5 : 5 + count]
    out, pages, queries, q_ref, m_in, acc_in, m_ref, acc_ref, v_ref, k_one, v_one, flag = refs[
        5 + count :
    ]
    sources = [
        (ref, i * rows, offset % shards)
        for ref, offs in zip(buffers, offsets)
        for i, offset in enumerate(offs)
        if offset is not None
    ]
    sources.sort(key=lambda source: -source[2] % shards)
    me = meta[0]
    live = me * rows < meta[1]
    per_piece = rows // PAGE_TOKENS

    def number_of(source):
        return lax.rem(me + source[2], shards)

    def needed(source):
        return number_of(source) < me

    def one_page(slot, carry):
        page = meta[2 + slot]
        pages[pl.ds(slot, 1)] = jnp.zeros((1, PAGE_TOKENS, 2 * HEAD_SIZE), jnp.bfloat16)
        owner = lax.div(page, per_piece)
        part = lax.rem(page, per_piece) * PAGE_TOKENS
        token = page * PAGE_TOKENS + lax.broadcasted_iota(
            jnp.int32, (PAGE_TOKENS, 2 * HEAD_SIZE), 0
        )
        for source in sources:
            here = jnp.logical_and(page >= 0, owner == number_of(source))

            @pl.when(here)
            def _():
                row0 = pl.multiple_of(source[1] + part, PAGE_TOKENS)
                block = source[0][pl.ds(row0, PAGE_TOKENS), :]
                kept = jnp.where(token < meta[1], block.astype(jnp.float32), 0.0)
                pages[pl.ds(slot, 1)] = kept.astype(jnp.bfloat16)[None]

        return carry

    lax.fori_loop(0, slots, one_page, 0)

    def keys_of(source):
        return source[0][source[1] : source[1] + rows, :HEAD_SIZE]

    def values_of(source):
        return values_across(source[0][source[1] : source[1] + rows, HEAD_SIZE:])

    @pl.when(jnp.logical_and(live, me < shards // 2))
    def _():
        q_ref[...] = q_first[...]
        m_in[...] = m_first[...]
        acc_in[...] = acc_first[...]

    @pl.when(jnp.logical_and(live, me >= shards // 2))
    def _():
        pltpu.sync_copy(queries_hbm, queries)
        own_tokens(queries, buffers[0], q_ref, m_in, acc_in, heads, rows)

    @pl.when(live)
    def _():
        acc_ref[...] = acc_in[...]
        m_ref[...] = m_in[...]

        def fast(part, worst):
            skip = []
            for i, source in enumerate(part):
                v_ref[i] = values_of(source)
                skip.append(jnp.where(needed(source), 0.0, -NEG_FILL))
            units = [(i, h) for i in range(len(part)) for h in range(heads)]

            def scored(unit):
                k = keys_of(part[unit[0]])
                return jnp.dot(k, q_ref[unit[1]], preferred_element_type=jnp.float32)

            ahead = [scored(u) for u in units[:AHEAD]]
            weights = []
            for n in range(len(units) + LAG):
                if n + AHEAD < len(units):
                    ahead.append(scored(units[n + AHEAD]))
                if n < len(units):
                    i, h = units[n]
                    t = ahead[n] * EXP2_SCALE - (m_in[h : h + 1, :] * EXP2_SCALE + skip[i])
                    ahead[n] = None
                    worst = jnp.maximum(worst, jnp.max(t, axis=0, keepdims=True))
                    weights.append(jnp.exp2(t).astype(jnp.bfloat16))
                if n >= LAG:
                    i, h = units[n - LAG]
                    got = jnp.dot(v_ref[i], weights[n - LAG], preferred_element_type=jnp.float32)
                    weights[n - LAG] = None
                    acc_ref[h] = acc_ref[h] + got
            return worst

        others = [source for source in sources if source[2] != 0]
        cut = v_ref.shape[0]
        first = len(others) % cut
        cuts = [0] * (first > 0) + list(range(first, len(others) + 1, cut))
        worst = jnp.zeros((1, rows), jnp.float32)
        for low, high in zip(cuts[:-1], cuts[1:]):
            part = others[low:high]
            some = needed(part[0])
            for source in part[1:]:
                some = jnp.logical_or(some, needed(source))
            worst = lax.cond(some, lambda w: fast(part, w), lambda w: w, worst)

        @pl.when(jnp.max(worst) > SHIFT_LIMIT)
        def _():
            acc_ref[...] = acc_in[...]

            def one(n, carry):
                flag[0] = 0
                for i, source in enumerate(others):

                    @pl.when(jnp.logical_and(n == i, needed(source)))
                    def _():
                        k_one[...] = keys_of(source)
                        v_one[...] = values_of(source)
                        flag[0] = 1

                @pl.when(flag[0] == 1)
                def _():
                    attend(q_ref, m_ref, acc_ref, k_one, v_one, heads)

                return carry

            lax.fori_loop(0, len(others), one, 0)

        row = me * rows + lax.broadcasted_iota(jnp.int32, (rows, HEAD_SIZE), 0)
        for h in range(heads):
            got = acc_ref[h, :HEAD_SIZE, :] / acc_ref[h, HEAD_SIZE : HEAD_SIZE + 1, :]
            got = jnp.where(row < meta[1], got.T, 0.0)
            out[:, h * HEAD_SIZE : (h + 1) * HEAD_SIZE] = got.astype(jnp.bfloat16)

    @pl.when(jnp.logical_not(live))
    def _():
        out[...] = jnp.zeros_like(out)


SMEM = pl.BlockSpec(memory_space=pltpu.SMEM)
VMEM = pl.BlockSpec(memory_space=pltpu.VMEM)
FAR = pl.BlockSpec(memory_space=pltpu.HBM)


def state_shapes(heads, rows):
    return (
        pltpu.VMEM((heads, HEAD_SIZE, rows), jnp.bfloat16),
        pltpu.VMEM((heads, rows), jnp.float32),
        pltpu.VMEM((heads, HEAD_SIZE + ONES_ROWS, rows), jnp.float32),
    )


def near(x):
    return pltpu.with_memory_space_constraint(x, pltpu.VMEM)


def far(x):
    return pltpu.with_memory_space_constraint(x, pltpu.HBM)


def cost(heads, rows, pieces):
    return pl.CostEstimate(
        flops=16 * heads * rows * rows * pieces * HEAD_SIZE,
        bytes_accessed=4 * 2**20,
        transcendentals=heads * rows * rows * pieces,
    )


def call_first(place, queries, keys, values, heads, rows, shards):
    return pl.pallas_call(
        lambda *r: first_kernel(*r, heads=heads, rows=rows, shards=shards),
        in_specs=[SMEM, FAR, FAR, FAR],
        out_specs=[VMEM] * 4,
        out_shape=(pltpu.VMEM((rows, 2 * HEAD_SIZE), jnp.bfloat16),) + state_shapes(heads, rows),
        scratch_shapes=[
            pltpu.VMEM(queries.shape, jnp.bfloat16),
            pltpu.SemaphoreType.DMA((2,)),
        ],
        cost_estimate=cost(heads, rows, 1),
        compiler_params=pltpu.CompilerParams(vmem_limit_bytes=16 * 2**20),
        name="first",
    )(place, far(queries), far(keys), far(values))


def call_rest(meta, queries, state, pieces, heads, rows, shards, slots):
    q_shape, m_shape, acc_shape = state_shapes(heads, rows)
    buffers = [buffer for buffer, unused2 in pieces]
    offsets = [offs for unused2, offs in pieces]
    wide = 2 * HEAD_SIZE

    def kernel(*refs):
        rest_kernel(*refs, offsets=offsets, heads=heads, rows=rows, shards=shards, slots=slots)

    return pl.pallas_call(
        kernel,
        in_specs=[SMEM, FAR] + [VMEM] * (3 + len(buffers)),
        out_specs=[VMEM] * 2,
        out_shape=(
            jax.ShapeDtypeStruct((rows, heads * HEAD_SIZE), jnp.bfloat16),
            jax.ShapeDtypeStruct((slots, PAGE_TOKENS, wide), jnp.bfloat16),
        ),
        scratch_shapes=[
            pltpu.VMEM(queries.shape, jnp.bfloat16),
            q_shape,
            m_shape,
            acc_shape,
            m_shape,
            acc_shape,
            pltpu.VMEM((PART, HEAD_SIZE + ONES_ROWS, rows), jnp.bfloat16),
            pltpu.VMEM((rows, HEAD_SIZE), jnp.bfloat16),
            pltpu.VMEM((HEAD_SIZE + ONES_ROWS, rows), jnp.bfloat16),
            pltpu.SMEM((1,), jnp.int32),
        ],
        cost_estimate=cost(heads, rows, shards - 1),
        compiler_params=pltpu.CompilerParams(vmem_limit_bytes=24 * 2**20),
        name="rest",
    )(meta, far(queries), *map(near, state), *map(near, buffers))


def facts(page_dest, owner, prompt_len, slots):
    flat = page_dest.reshape(-1)
    order = jnp.arange(flat.shape[0], dtype=jnp.int32)
    before = (flat[:, None] == flat[None, :]) & (order[None, :] < order[:, None])
    rank = jnp.sum(before.astype(jnp.int32), axis=1)
    slot = jnp.arange(slots, dtype=jnp.int32)
    match = (flat[:, None] == owner) & (rank[:, None] == slot[None, :])
    page = jnp.max(jnp.where(match, order[:, None], -1), axis=0)
    return jnp.concatenate([jnp.stack([owner, prompt_len[0]]), page]).astype(jnp.int32)


def local(queries, keys, values, prompt_len, page_dest):
    rows = queries.shape[0]
    heads = queries.shape[1] // keys.shape[1]
    shards = page_dest.shape[0]
    slots = 2 * page_dest.shape[1]
    meta = facts(page_dest, lax.axis_index("seq"), prompt_len, slots)

    def moved(x, by):
        pairs = [(i, (i + by) % shards) for i in range(shards)]
        return lax.ppermute(x, "seq", pairs)

    place = lax.axis_index("seq").astype(jnp.int32).reshape(1)
    own, *state = call_first(place, queries, keys, values, heads, rows, shards)
    up = down = own
    pieces, seen = [], set()

    def keep(buffer, offs):
        fresh = []
        for offset in offs:
            fresh.append(None if offset % shards in seen else offset)
            seen.add(offset % shards)
        pieces.append((buffer, fresh))

    keep(own, [0])
    steps = shards // 6
    batch = [(own, 0)]
    for t in range(1, steps + 1):
        up, down = moved(up, 3), moved(down, -3)
        keep(up, [-3 * t])
        keep(down, [3 * t])
        batch += [(up, -3 * t), (down, 3 * t)]
        for by in (1, -1):
            part = [(x, o - by) for x, o in batch if t < steps or (o - by) % shards not in seen]
            joined = jnp.concatenate([x for x, unused in part], axis=0)
            keep(moved(joined, by), [o for unused, o in part])
        batch = []
    attended, pages = call_rest(meta, queries, state, pieces, heads, rows, shards, slots)
    return attended, pages


def solution(mesh):
    return jax.shard_map(
        local,
        mesh=mesh,
        in_specs=(
            P(("groups", "seq"), "head"),
            P(("groups", "seq"), "head"),
            P(("groups", "seq"), "head"),
            P("groups"),
            P("groups", None),
        ),
        out_specs=(P(("groups", "seq"), "head"), P(("groups", "seq"), None, "head")),
        check_vma=False,
    )
```

```python
import math

import jax
import jax.numpy as jnp
from jax import lax
from jax.experimental import pallas as pl
from jax.experimental.pallas import tpu as pltpu
from jax.sharding import PartitionSpec as P

HEAD_SIZE = 128
PAGE_TOKENS = 128
ONES_ROWS = 16
NEG_FILL = -1e30
SHIFT_LIMIT = 64.0
AHEAD = 3
LAG = 1
PART = 4
EXP2_SCALE = math.log2(math.e) / math.sqrt(HEAD_SIZE)


def values_across(v):
    turned = v.astype(jnp.float32).T.astype(jnp.bfloat16)
    return jnp.concatenate([turned, jnp.ones((ONES_ROWS, v.shape[0]), jnp.bfloat16)], axis=0)


def attend(q_ref, m_ref, acc_ref, k_ref, v_ref, heads):
    for h in range(heads):
        s = jnp.dot(k_ref[...], q_ref[h], preferred_element_type=jnp.float32)
        old = m_ref[h : h + 1, :]
        new = jnp.maximum(old, jnp.max(s, axis=0, keepdims=True))
        shift = new * EXP2_SCALE
        w = jnp.exp2(s * EXP2_SCALE - shift).astype(jnp.bfloat16)
        got = jnp.dot(v_ref[...], w, preferred_element_type=jnp.float32)
        acc_ref[h] = acc_ref[h] * jnp.exp2(old * EXP2_SCALE - shift) + got
        m_ref[h : h + 1, :] = new


def own_tokens(queries, piece, q_ref, m_ref, acc_ref, heads, rows):
    k = piece[:, :HEAD_SIZE]
    v = values_across(piece[:, HEAD_SIZE:])
    key = lax.broadcasted_iota(jnp.int32, (rows, rows), 0)
    query = lax.broadcasted_iota(jnp.int32, (rows, rows), 1)
    allowed = key <= query
    for h in range(heads):
        q = queries[:, h * HEAD_SIZE : (h + 1) * HEAD_SIZE]
        q = q.astype(jnp.float32).T.astype(jnp.bfloat16)
        q_ref[h] = q
        s = jnp.dot(k, q, preferred_element_type=jnp.float32)
        s = jnp.where(allowed, s, NEG_FILL)
        new = jnp.max(s, axis=0, keepdims=True)
        w = jnp.exp2((s - new) * EXP2_SCALE).astype(jnp.bfloat16)
        m_ref[h : h + 1, :] = new
        acc_ref[h] = jnp.dot(v, w, preferred_element_type=jnp.float32)


def first_kernel(
    place, queries_hbm, keys, values, piece, q_ref, m_ref, acc_ref, queries, sems,
    *, heads, rows, shards,
):
    key_copy = pltpu.make_async_copy(keys, piece.at[:, pl.ds(0, HEAD_SIZE)], sems.at[0])
    value_copy = pltpu.make_async_copy(values, piece.at[:, pl.ds(HEAD_SIZE, HEAD_SIZE)], sems.at[1])
    key_copy.start()
    value_copy.start()
    key_copy.wait()
    value_copy.wait()

    @pl.when(place[0] < shards // 2)
    def _():
        pltpu.sync_copy(queries_hbm, queries)
        own_tokens(queries, piece, q_ref, m_ref, acc_ref, heads, rows)


def rest_kernel(*refs, offsets, heads, rows, shards, slots, last):
    count = len(offsets)
    if last:
        meta, q_ref, m_in, acc_in, pages_in = refs[:5]
        out, pages, m_ref, acc_ref, v_ref, k_one, v_one, flag = refs[5 + count :]
        pages[...] = pages_in[...]
    else:
        meta, queries_hbm, q_first, m_first, acc_first = refs[:5]
        q_ref, m_ref, acc_ref, pages, queries, m_in, acc_in, v_ref, k_one, v_one, flag = refs[
            5 + count :
        ]
        pages[...] = jnp.zeros_like(pages)
    buffers = refs[5 : 5 + count]
    sources = [
        (ref, i * rows, offset % shards)
        for ref, offs in zip(buffers, offsets)
        for i, offset in enumerate(offs)
        if offset is not None
    ]
    sources.sort(key=lambda source: -source[2] % shards)
    me = meta[0]
    live = me * rows < meta[1]
    per_piece = rows // PAGE_TOKENS

    def number_of(source):
        return lax.rem(me + source[2], shards)

    def needed(source):
        return number_of(source) < me

    def one_page(slot, carry):
        page = meta[2 + slot]
        owner = lax.div(page, per_piece)
        part = lax.rem(page, per_piece) * PAGE_TOKENS
        token = page * PAGE_TOKENS + lax.broadcasted_iota(
            jnp.int32, (PAGE_TOKENS, 2 * HEAD_SIZE), 0
        )
        for source in sources:
            here = jnp.logical_and(page >= 0, owner == number_of(source))

            @pl.when(here)
            def _():
                row0 = pl.multiple_of(source[1] + part, PAGE_TOKENS)
                block = source[0][pl.ds(row0, PAGE_TOKENS), :]
                kept = jnp.where(token < meta[1], block.astype(jnp.float32), 0.0)
                pages[pl.ds(slot, 1)] = kept.astype(jnp.bfloat16)[None]

        return carry

    lax.fori_loop(0, slots, one_page, 0)

    def keys_of(source):
        return source[0][source[1] : source[1] + rows, :HEAD_SIZE]

    def values_of(source):
        return values_across(source[0][source[1] : source[1] + rows, HEAD_SIZE:])

    if not last:

        @pl.when(jnp.logical_and(live, me < shards // 2))
        def _():
            q_ref[...] = q_first[...]
            m_in[...] = m_first[...]
            acc_in[...] = acc_first[...]

        @pl.when(jnp.logical_and(live, me >= shards // 2))
        def _():
            pltpu.sync_copy(queries_hbm, queries)
            own_tokens(queries, buffers[0], q_ref, m_in, acc_in, heads, rows)

    @pl.when(live)
    def _():
        acc_ref[...] = acc_in[...]
        m_ref[...] = m_in[...]

        def fast(part, worst):
            skip = []
            for i, source in enumerate(part):
                v_ref[i] = values_of(source)
                skip.append(jnp.where(needed(source), 0.0, -NEG_FILL))
            units = [(i, h) for i in range(len(part)) for h in range(heads)]

            def scored(unit):
                k = keys_of(part[unit[0]])
                return jnp.dot(k, q_ref[unit[1]], preferred_element_type=jnp.float32)

            ahead = [scored(u) for u in units[:AHEAD]]
            weights = []
            for n in range(len(units) + LAG):
                if n + AHEAD < len(units):
                    ahead.append(scored(units[n + AHEAD]))
                if n < len(units):
                    i, h = units[n]
                    t = ahead[n] * EXP2_SCALE - (m_in[h : h + 1, :] * EXP2_SCALE + skip[i])
                    ahead[n] = None
                    worst = jnp.maximum(worst, jnp.max(t, axis=0, keepdims=True))
                    weights.append(jnp.exp2(t).astype(jnp.bfloat16))
                if n >= LAG:
                    i, h = units[n - LAG]
                    got = jnp.dot(v_ref[i], weights[n - LAG], preferred_element_type=jnp.float32)
                    weights[n - LAG] = None
                    acc_ref[h] = acc_ref[h] + got
            return worst

        others = [source for source in sources if source[2] != 0]
        cut = v_ref.shape[0]
        first = len(others) % cut
        cuts = [0] * (first > 0) + list(range(first, len(others) + 1, cut))
        worst = jnp.zeros((1, rows), jnp.float32)
        for low, high in zip(cuts[:-1], cuts[1:]):
            part = others[low:high]
            some = needed(part[0])
            for source in part[1:]:
                some = jnp.logical_or(some, needed(source))
            worst = lax.cond(some, lambda w: fast(part, w), lambda w: w, worst)

        @pl.when(jnp.max(worst) > SHIFT_LIMIT)
        def _():
            acc_ref[...] = acc_in[...]

            def one(n, carry):
                flag[0] = 0
                for i, source in enumerate(others):

                    @pl.when(jnp.logical_and(n == i, needed(source)))
                    def _():
                        k_one[...] = keys_of(source)
                        v_one[...] = values_of(source)
                        flag[0] = 1

                @pl.when(flag[0] == 1)
                def _():
                    attend(q_ref, m_ref, acc_ref, k_one, v_one, heads)

                return carry

            lax.fori_loop(0, len(others), one, 0)

        if last:
            row = me * rows + lax.broadcasted_iota(jnp.int32, (rows, HEAD_SIZE), 0)
            for h in range(heads):
                got = acc_ref[h, :HEAD_SIZE, :] / acc_ref[h, HEAD_SIZE : HEAD_SIZE + 1, :]
                got = jnp.where(row < meta[1], got.T, 0.0)
                out[:, h * HEAD_SIZE : (h + 1) * HEAD_SIZE] = got.astype(jnp.bfloat16)

    if last:

        @pl.when(jnp.logical_not(live))
        def _():
            out[...] = jnp.zeros_like(out)


SMEM = pl.BlockSpec(memory_space=pltpu.SMEM)
VMEM = pl.BlockSpec(memory_space=pltpu.VMEM)
FAR = pl.BlockSpec(memory_space=pltpu.HBM)


def state_shapes(heads, rows):
    return (
        pltpu.VMEM((heads, HEAD_SIZE, rows), jnp.bfloat16),
        pltpu.VMEM((heads, rows), jnp.float32),
        pltpu.VMEM((heads, HEAD_SIZE + ONES_ROWS, rows), jnp.float32),
    )


def near(x):
    return pltpu.with_memory_space_constraint(x, pltpu.VMEM)


def far(x):
    return pltpu.with_memory_space_constraint(x, pltpu.HBM)


def cost(heads, rows, pieces):
    return pl.CostEstimate(
        flops=16 * heads * rows * rows * pieces * HEAD_SIZE,
        bytes_accessed=4 * 2**20,
        transcendentals=heads * rows * rows * pieces,
    )


def call_first(place, queries, keys, values, heads, rows, shards):
    return pl.pallas_call(
        lambda *r: first_kernel(*r, heads=heads, rows=rows, shards=shards),
        in_specs=[SMEM, FAR, FAR, FAR],
        out_specs=[VMEM] * 4,
        out_shape=(pltpu.VMEM((rows, 2 * HEAD_SIZE), jnp.bfloat16),) + state_shapes(heads, rows),
        scratch_shapes=[
            pltpu.VMEM(queries.shape, jnp.bfloat16),
            pltpu.SemaphoreType.DMA((2,)),
        ],
        cost_estimate=cost(heads, rows, 1),
        compiler_params=pltpu.CompilerParams(vmem_limit_bytes=16 * 2**20),
        name="first",
    )(place, far(queries), far(keys), far(values))


def call_rest(meta, given, pieces, heads, rows, shards, slots, last):
    q_shape, m_shape, acc_shape = state_shapes(heads, rows)
    buffers = [buffer for buffer, unused in pieces]
    offsets = [offs for unused, offs in pieces]
    pages = (slots, PAGE_TOKENS, 2 * HEAD_SIZE)
    if last:
        out_shape = (
            jax.ShapeDtypeStruct((rows, heads * HEAD_SIZE), jnp.bfloat16),
            jax.ShapeDtypeStruct(pages, jnp.bfloat16),
        )
        scratch = [m_shape, acc_shape]
        operands = [near(x) for x in given]
    else:
        out_shape = (q_shape, m_shape, acc_shape, pltpu.VMEM(pages, jnp.bfloat16))
        scratch = [pltpu.VMEM(given[0].shape, jnp.bfloat16), m_shape, acc_shape]
        operands = [far(given[0])] + [near(x) for x in given[1:]]

    def kernel(*refs):
        rest_kernel(
            *refs, offsets=offsets, heads=heads, rows=rows, shards=shards, slots=slots, last=last
        )

    return pl.pallas_call(
        kernel,
        in_specs=[SMEM, VMEM if last else FAR] + [VMEM] * (3 + len(buffers)),
        out_specs=[VMEM] * len(out_shape),
        out_shape=out_shape,
        scratch_shapes=scratch
        + [
            pltpu.VMEM((PART, HEAD_SIZE + ONES_ROWS, rows), jnp.bfloat16),
            pltpu.VMEM((rows, HEAD_SIZE), jnp.bfloat16),
            pltpu.VMEM((HEAD_SIZE + ONES_ROWS, rows), jnp.bfloat16),
            pltpu.SMEM((1,), jnp.int32),
        ],
        cost_estimate=cost(heads, rows, sum(len(offs) for offs in offsets)),
        compiler_params=pltpu.CompilerParams(vmem_limit_bytes=24 * 2**20),
        name="last" if last else "rest",
    )(meta, *operands, *map(near, buffers))


def facts(page_dest, owner, prompt_len, slots):
    flat = page_dest.reshape(-1)
    order = jnp.arange(flat.shape[0], dtype=jnp.int32)
    before = (flat[:, None] == flat[None, :]) & (order[None, :] < order[:, None])
    rank = jnp.sum(before.astype(jnp.int32), axis=1)
    slot = jnp.arange(slots, dtype=jnp.int32)
    match = (flat[:, None] == owner) & (rank[:, None] == slot[None, :])
    page = jnp.max(jnp.where(match, order[:, None], -1), axis=0)
    return jnp.concatenate([jnp.stack([owner, prompt_len[0]]), page]).astype(jnp.int32)


def local(queries, keys, values, prompt_len, page_dest):
    rows = queries.shape[0]
    heads = queries.shape[1] // keys.shape[1]
    shards = page_dest.shape[0]
    slots = 2 * page_dest.shape[1]
    meta = facts(page_dest, lax.axis_index("seq"), prompt_len, slots)

    def moved(x, by):
        pairs = [(i, (i + by) % shards) for i in range(shards)]
        return lax.ppermute(x, "seq", pairs)

    place = lax.axis_index("seq").astype(jnp.int32).reshape(1)
    own, *state = call_first(place, queries, keys, values, heads, rows, shards)
    up = down = own
    pieces, seen = [], set()

    def keep(buffer, offs):
        fresh = []
        for offset in offs:
            fresh.append(None if offset % shards in seen else offset)
            seen.add(offset % shards)
        pieces.append((buffer, fresh))

    keep(own, [0])
    steps = shards // 6
    batch = [(own, 0)]
    for t in range(1, steps + 1):
        up, down = moved(up, 3), moved(down, -3)
        keep(up, [-3 * t])
        keep(down, [3 * t])
        batch += [(up, -3 * t), (down, 3 * t)]
        for by in (1, -1):
            part = [(x, o - by) for x, o in batch if t < steps or (o - by) % shards not in seen]
            joined = jnp.concatenate([x for x, unused in part], axis=0)
            keep(moved(joined, by), [o for unused, o in part])
        batch = []
    meta, unused, unused2 = lax.optimization_barrier((meta, up, down))
    early, late = pieces[:-6] + pieces[-4:-2], pieces[-6:-4] + pieces[-2:]
    given = call_rest(meta, (queries, *state), early, heads, rows, shards, slots, last=False)
    attended, pages = call_rest(meta, given, late, heads, rows, shards, slots, last=True)
    return attended, pages


def solution(mesh):
    return jax.shard_map(
        local,
        mesh=mesh,
        in_specs=(
            P(("groups", "seq"), "head"),
            P(("groups", "seq"), "head"),
            P(("groups", "seq"), "head"),
            P("groups"),
            P("groups", None),
        ),
        out_specs=(P(("groups", "seq"), "head"), P(("groups", "seq"), None, "head")),
        check_vma=False,
    )
```
